32 devices in a mesh: rows: 8 (over z, y), sub: 4 (over x, core).
Axes of the slice: x: 2, y: 2, z: 4, core: 2. Of those that a mesh axis runs over, the one named last changes fastest.
Arguments:
- snapshots: float32 [513, 32768], P(None, ('rows', 'sub')), may hold values from -6 to 6
- start: float32 [512, 64], replicated, may hold values from -6 to 6
Outputs:
- modes: float32 [128, 32768], P(None, ('rows', 'sub'))
- operator: float32 [128, 128], replicated
- coefficients: float32 [128, 513], replicated
The draws below stay inside these ranges and needn't reach their ends.
All inputs are finite; a program needn't handle non-finite values.
Results may differ from the reference program's by a relative error of at most 0.0003.
Values sent between devices are 32-bit elements; how exact they have to be, the bound alone decides.
A program may use at most 64 MiB of HBM per device.

```python
import jax
import jax.numpy as jnp
from jax import lax

SNAPS = 513
BLOCK = 64
STEPS = 2
RANK = 128
CELLS = 32768


def shard_levels(rng, shape, cuts, least, high):
    factor_of, own = 1.0, jax.random.fold_in(rng, 6)
    for position, blocks in cuts:
        steps = jnp.exp(jax.random.uniform(jax.random.fold_in(own, position), (blocks,), jnp.float32, least / len(cuts), high / len(cuts)))
        factor_of = factor_of * jnp.repeat(steps, shape[position] // blocks).reshape([-1 if axis == position else 1 for axis in range(len(shape))])
    return factor_of


def centred(rng, shape, scale, bound, cuts=(), kind=jnp.bfloat16):
    drawn = scale * jax.random.normal(rng, shape, jnp.float32)
    if cuts:
        drawn = drawn * shard_levels(rng, shape, cuts, -0.22, 0.18)
    return jnp.clip(drawn, -bound, bound).astype(kind)


def setup_inputs(seed: int = 0) -> dict:
    key_list = jax.random.split(jax.random.key(seed), 3)
    return {
        "snapshots": centred(key_list[0], (SNAPS, CELLS), 1.0, 6.0, ((1, 32),), jnp.float32),
        "start": centred(key_list[1], (SNAPS - 1, BLOCK), 1.0, 6.0, (), jnp.float32),
    }


def cross_cells(left, right):
    return lax.dot_general(left.astype(jnp.float32), right.astype(jnp.float32), (((1,), (1,)), ((), ())), precision=lax.Precision.HIGHEST, preferred_element_type=jnp.float32)

def matmul(left, right):
    return jnp.dot(left.astype(jnp.float32), right.astype(jnp.float32), precision=lax.Precision.HIGHEST, preferred_element_type=jnp.float32)

def factor_inverse(gram_block):
    factor = jnp.linalg.cholesky(gram_block)
    identity = jnp.eye(gram_block.shape[0], dtype=jnp.float32)
    inverse = jax.scipy.linalg.solve_triangular(factor, identity, lower=True)
    return (factor, inverse)

def orthonormal_columns(matrix):
    factor, inverse = factor_inverse(matmul(matrix.T, matrix))
    return matmul(matrix, inverse.T)

def reference(snapshots, start):
    width = start.shape[1]
    count = snapshots.shape[0]
    right_block = orthonormal_columns(start)
    right_blocks = [right_block]
    left_blocks = []
    columns = []
    for step in range(STEPS):
        padded = jnp.concatenate([right_block, jnp.zeros((1, width), jnp.float32)], 0)
        image = matmul(padded.T, snapshots)
        pieces = []
        if step > 0:
            earlier = jnp.concatenate(left_blocks, 0)
            coupling = cross_cells(earlier, image)
            image = image - matmul(coupling.T, earlier)
            pieces.append(coupling)
        factor, inverse = factor_inverse(cross_cells(image, image))
        left_blocks.append(matmul(inverse, image))
        pieces.append(factor.T)
        below = RANK - (step + 1) * width
        if below > 0:
            pieces.append(jnp.zeros((below, width), jnp.float32))
        columns.append(jnp.concatenate(pieces, 0))
        if step < STEPS - 1:
            back_sum = cross_cells(snapshots, left_blocks[-1])[:count - 1]
            basis = jnp.concatenate(right_blocks, 1)
            back_sum = back_sum - matmul(basis, matmul(basis.T, back_sum))
            right_block = orthonormal_columns(back_sum)
            right_blocks.append(right_block)
    triangle = jnp.concatenate(columns, 1)
    inverse_tri = jax.scipy.linalg.solve_triangular(triangle, jnp.eye(RANK, dtype=jnp.float32), lower=False)
    basis = jnp.concatenate(right_blocks, 1)
    shifted = jnp.concatenate([jnp.zeros((1, RANK), jnp.float32), basis], 0)
    advanced = matmul(shifted.T, snapshots)
    left_all = jnp.concatenate(left_blocks, 0)
    operator = matmul(cross_cells(left_all, advanced), inverse_tri)
    scale = jnp.sqrt(jnp.asarray(CELLS, jnp.float32))
    modes = scale * matmul(inverse_tri.T, advanced)
    mode_gram = cross_cells(modes, modes)
    mode_rhs = cross_cells(modes, snapshots)
    coefficients = jax.scipy.linalg.cho_solve((jnp.linalg.cholesky(mode_gram), True), mode_rhs)
    return (modes, operator, coefficients)
```

```python
import functools

import jax
import jax.numpy as jnp
from jax import lax
from jax.experimental import pallas as pl
from jax.experimental.pallas import tpu as pltpu
from jax.sharding import PartitionSpec as P

HIGHEST = lax.Precision.HIGHEST
TILE = 8
LANES = 128
PANEL = 4


def dot(left, right, dims):
    return lax.dot_general(
        left, right, (dims, ((), ())), precision=HIGHEST, preferred_element_type=jnp.float32
    )


def nn(left, right):
    return dot(left, right, ((1,), (0,)))


def nt(left, right):
    return dot(left, right, ((1,), (1,)))


def tn(left, right):
    return dot(left, right, ((0,), (0,)))


def iotas(rows, lanes):
    return (
        lax.broadcasted_iota(jnp.int32, (rows, lanes), 0),
        lax.broadcasted_iota(jnp.int32, (rows, lanes), 1),
    )


def eliminate(blocks, offset, width):
    tiles = [[b[t : t + TILE] for t in range(0, width, TILE)] for b in blocks]
    shape = (TILE, 2 * width)
    sub = lax.broadcasted_iota(jnp.int32, shape, 0)
    for j in range(0, width, PANEL):
        home, inner = j // TILE, j % TILE
        at = offset + j
        live = range(home, width // TILE)
        for own in tiles:
            cols = [
                {t: jnp.broadcast_to(own[t][:, at + q : at + q + 1], shape) for t in live} for q in range(PANEL)
            ]
            rows = [jnp.broadcast_to(own[home][inner + q : inner + q + 1], shape) for q in range(PANEL)]
            small = [
                [
                    jnp.broadcast_to(cols[c][home][inner + q : inner + q + 1], shape) if c >= q else None
                    for c in range(PANEL)
                ]
                for q in range(PANEL)
            ]
            for q in range(PANEL):
                inverse = 1.0 / small[q][q]
                factor = {t: cols[q][t] * inverse for t in live}
                factor[home] = jnp.where(sub > inner + q, factor[home], 0.0)
                for c in range(q + 1, PANEL):
                    ratio = small[q][c] * inverse
                    for e in range(c, PANEL):
                        small[c][e] = small[c][e] - ratio * small[q][e]
                    rows[c] = rows[c] - ratio * rows[q]
                    for t in live:
                        cols[c][t] = cols[c][t] - factor[t] * small[q][c]
                for t in live:
                    own[t] = own[t] - factor[t] * rows[q]
    row, lane = iotas(width, 2 * width)
    place = lane - offset
    inside = (place >= 0) & (place < width)
    out = []
    for own in tiles:
        whole = jnp.concatenate(own, 0)
        pivot = jnp.sum(jnp.where(place == row, whole, 0.0), axis=1, keepdims=True)
        whole = whole * (1.0 / jnp.sqrt(pivot))
        out.append(jnp.where(inside & (place < row), 0.0, whole))
    return out


def plan(past):
    blocks = [(r, c) for r in range(past // LANES) for c in range(r, past // LANES)]
    tails = list(range(past // LANES + 1))
    cut = (len(blocks) + 1) // 2
    keep = len(tails) - 1
    lengths = (cut * LANES + keep * TILE, (len(blocks) - cut) * LANES + TILE)
    half = -(-max(lengths) // (4 * TILE)) * 4 * TILE
    where = {}
    for n, block in enumerate(blocks):
        where[block] = n * LANES if n < cut else half + (n - cut) * LANES
    tail_rows = [cut * LANES + TILE * c for c in range(keep)] + [half + (len(blocks) - cut) * LANES]
    return half, where, tail_rows


def split(block):
    high = block.astype(jnp.bfloat16)
    return high, (block - high.astype(jnp.float32)).astype(jnp.bfloat16)


def fast_nt(left, right, dims=((1,), (1,))):
    def one(a, b):
        return lax.dot_general(a, b, (dims, ((), ())), preferred_element_type=jnp.float32)

    return one(left[0], right[0]) + (one(left[0], right[1]) + one(left[1], right[0]))


def gram_kernel(sizes, snap_ref, start_ref, out_ref, right_ref, acc, full, got0, got1, got2, got3, send_sems, recv_sems):
    rows_total, sub_total = sizes
    count = snap_ref.shape[0]
    past = count - 1
    half, where, tail_rows = plan(past)
    row, sub = lax.axis_index("rows"), lax.axis_index("sub")

    def bit(index, k):
        return lax.rem(index // (1 << k), 2)

    def step(index, k):
        return (1 - 2 * bit(index, k)) * (1 << k)

    core = bit(sub, 0)
    bx, by = bit(sub, 1), bit(row, 0)
    dx, dy = step(sub, 1), step(row, 0)
    other = 1 - core
    halvings = [
        ((row, sub + step(sub, 0)), core),
        ((row + core * dy, sub + other * dx), other * bx + core * by),
        ((row + other * dy, sub + core * dx), core * bx + other * by),
    ]
    whole = [(row, sub + step(sub, k)) for k in range(2, sub_total.bit_length() - 1)]
    whole += [(row + step(row, k), sub) for k in range(1, rows_total.bit_length() - 1)]
    partners = [h[0] for h in halvings] + whole

    barrier = pltpu.get_barrier_semaphore()
    for partner in partners:
        pl.semaphore_signal(barrier, inc=1, device_id=partner, device_id_type=pl.DeviceIdType.MESH)

    for (r, c), place in where.items():
        if r == c:
            panel = fast_nt(split(snap_ref[r * LANES : (r + 1) * LANES]), split(snap_ref[r * LANES : past]))
        acc[place : place + LANES] = panel[:, (c - r) * LANES : (c - r + 1) * LANES]
    last = jnp.concatenate([snap_ref[past:count], jnp.zeros((TILE - 1, snap_ref.shape[1]), jnp.float32)], 0)
    tail = fast_nt(split(last), split(snap_ref[:past]))
    for c, place in enumerate(tail_rows[:-1]):
        acc[place : place + TILE] = tail[:, c * LANES : (c + 1) * LANES]
    corner = jnp.sum(last * last, axis=1, keepdims=True)
    lane = lax.broadcasted_iota(jnp.int32, (TILE, LANES), 1)
    acc[tail_rows[-1] : tail_rows[-1] + TILE] = jnp.where(lane == 0, corner, 0.0)
    end0, end1 = tail_rows[-2] + TILE, tail_rows[-1] + TILE
    if end0 < half:
        acc[end0:half] = jnp.zeros((half - end0, LANES), jnp.float32)
    if end1 < 2 * half:
        acc[end1 : 2 * half] = jnp.zeros((2 * half - end1, LANES), jnp.float32)

    pl.semaphore_wait(barrier, len(partners))

    def orthonormal():
        start = start_ref[...]
        width = start_ref.shape[0]
        eye_row, eye_lane = iotas(width, 2 * width)
        eye_right = (eye_lane - width == eye_row).astype(jnp.float32)
        block = jnp.where(eye_lane < width, nt(start, twice(start)), eye_right)
        (first,) = eliminate([block], 0, width)
        right_ref[...] = dot(start, twice(first[:, width:]), ((0,), (1,)))

    def exchange(n, src, dst, partner, beside=None):
        copy = pltpu.make_async_remote_copy(
            src_ref=src,
            dst_ref=dst,
            send_sem=send_sems.at[n],
            recv_sem=recv_sems.at[n],
            device_id=partner,
            device_id_type=pl.DeviceIdType.MESH,
        )
        copy.start()
        if beside is not None:
            beside()
        copy.wait()

    def rows_at(start, length):
        return pl.ds(pl.multiple_of(start, TILE), length)

    offset, length, n = 0, half, 0
    trail = []
    for (partner, side), got in zip(halvings, (got0, got1, got2)):
        beside = None
        exchange(n, acc.at[rows_at(offset + (1 - side) * length, length)], got, partner, beside)
        offset = offset + side * length
        mine = rows_at(offset, length)
        acc[mine] = acc[mine] + got[...]
        trail.append((partner, offset, length))
        length, n = length // 2, n + 1
    length = length * 2
    mine = rows_at(offset, length)
    for k, partner in enumerate(whole):
        exchange(n, acc.at[mine], got3.at[k], partner, orthonormal if k == len(whole) - 1 else None)
        n += 1
        target = full if k == len(whole) - 1 else acc
        target[mine] = acc[mine] + got3[k]
    for partner, begin, span in reversed(trail):
        part = rows_at(begin, span)
        exchange(n, full.at[part], full.at[part], partner)
        n += 1
    out_ref[...] = full[...]


def unpack(packed_ref, gram_ref, past):
    _, where, tail_rows = plan(past)
    gram_ref[past:] = jnp.zeros((gram_ref.shape[0] - past, gram_ref.shape[1]), jnp.float32)
    for (r, c), place in where.items():
        block = packed_ref[place : place + LANES]
        gram_ref[r * LANES : (r + 1) * LANES, c * LANES : (c + 1) * LANES] = block
        if r != c:
            gram_ref[c * LANES : (c + 1) * LANES, r * LANES : (r + 1) * LANES] = block.T
    extra = gram_ref.shape[1] - past
    lane = lax.broadcasted_iota(jnp.int32, (LANES, extra), 1)
    for c, place in enumerate(tail_rows):
        block = packed_ref[place : place + TILE]
        if c * LANES < past:
            gram_ref[past : past + TILE, c * LANES : (c + 1) * LANES] = block
            column = jnp.concatenate([block, jnp.zeros((LANES - TILE, LANES), jnp.float32)], 0).T
            gram_ref[c * LANES : (c + 1) * LANES, past:] = jnp.where(lane == 0, column[:, :extra], 0.0)
        else:
            gram_ref[past : past + TILE, past:] = block[:, :extra]


def twice(block):
    return jnp.concatenate([block, block], 0)


def chain_kernel(total_cells, snap_ref, packed_ref, right_ref, modes_ref, operator_ref, coef_ref, z_ref, gram_ref):
    past, order = right_ref.shape
    width = order // 2
    count = past + 1
    padded = gram_ref.shape[0]
    unpack(packed_ref, gram_ref, past)
    row, lane = iotas(width, order)
    low = lane < width
    eye_left = (lane == row).astype(jnp.float32)
    eye_right = (lane - width == row).astype(jnp.float32)

    def lows(rows):
        return lax.broadcasted_iota(jnp.int32, (rows, order), 1) < width

    def shift(block):
        z_ref[...] = jnp.zeros_like(z_ref)
        z_ref[1 : past + 1] = block
        return z_ref[...]

    def pad(block):
        return jnp.concatenate([block, jnp.zeros((padded - past, order), jnp.float32)], 0)

    right = right_ref[...]
    rp, rs = pad(right), shift(right)
    pair = jnp.concatenate([rp, rs], 1)
    gram = split(gram_ref[...])
    gpair = fast_nt(gram, split(pair), ((1,), (0,)))
    image_gram = tn(right, gpair[:past, :order])
    adv_gram = tn(rs, gpair[:, order:])
    residual = gpair[:past, :order] - nn(jnp.where(lows(past), right, 0.0), image_gram)
    m1, h1 = eliminate(
        [jnp.where(low, image_gram[:width], eye_right), jnp.where(low, adv_gram[:width], eye_right)], 0, width
    )
    second = nt(jnp.where(lows(past), 0.0, residual), twice(m1))
    basis = jnp.where(lows(past), right, second)
    zp, zs = pad(basis), shift(basis)
    zpair = jnp.concatenate([zp, zs], 1)
    gz = fast_nt(gram, split(zpair), ((1,), (0,)))
    prods = tn(zpair, gz)
    kmat, fmat, hmat = prods[:order, :order], prods[:order, order:], prods[order:, order:]

    def reduce_first(first, mat):
        rolled = pltpu.roll(first, width, 1)
        n1 = jnp.concatenate([jnp.where(low, rolled, 0.0), eye_right], 0)
        mid = nt(nn(n1, mat), n1)
        couple = jnp.where(low, 0.0, mid[:width])
        corner = mid[width:] - tn(couple, couple)[width:]
        tail = nn(jnp.where(low, -mid[width:], eye_right), n1)
        return n1, couple, jnp.where(low, eye_left, corner), tail

    kn1, kcouple, kcorner, ktail = reduce_first(m1, kmat)
    hn1, _, hcorner, htail = reduce_first(h1, hmat)
    m2, h2 = eliminate([kcorner, hcorner], width, width)
    ninv = jnp.concatenate([kn1[:width], nn(m2[:, :width], ktail)], 0)
    hinv = jnp.concatenate([hn1[:width], nn(h2[:, :width], htail)], 0)
    triangle = jnp.concatenate([jnp.where(low, m1, kcouple), jnp.where(low, 0.0, m2)], 0)

    operator_ref[...] = nt(nn(ninv, fmat), ninv)
    scale = jnp.sqrt(jnp.asarray(total_cells, jnp.float32))
    solver = nn(nt(triangle, hinv), hinv) * (1.0 / scale)
    coef_ref[...] = nt(gz[:, order:], solver)[:count]
    weights = nt(ninv, zs) * scale
    bulk = fast_nt(split(weights[:, :past]), split(snap_ref[:past]), ((1,), (0,)))
    modes_ref[...] = bulk + weights[:, past:count] * snap_ref[past:count]


def shards(sizes, snapshots, start):
    count, cells = snapshots.shape
    past, width = start.shape
    order = 2 * width
    padded = -(-count // TILE) * TILE
    vmem = pl.BlockSpec(memory_space=pltpu.VMEM)
    half, _, _ = plan(past)
    copies = (sizes[0] * sizes[1]).bit_length() - 1
    packed, right = pl.pallas_call(
        functools.partial(gram_kernel, sizes),
        out_shape=(
            jax.ShapeDtypeStruct((2 * half, LANES), jnp.float32),
            jax.ShapeDtypeStruct((past, order), jnp.float32),
        ),
        in_specs=[vmem] * 2,
        out_specs=(vmem,) * 2,
        scratch_shapes=[
            pltpu.VMEM((2 * half, LANES), jnp.float32),
            pltpu.VMEM((2 * half, LANES), jnp.float32),
            pltpu.VMEM((half, LANES), jnp.float32),
            pltpu.VMEM((half // 2, LANES), jnp.float32),
            pltpu.VMEM((half // 4, LANES), jnp.float32),
            pltpu.VMEM((copies - 3, half // 4, LANES), jnp.float32),
            pltpu.SemaphoreType.DMA((copies + 3,)),
            pltpu.SemaphoreType.DMA((copies + 3,)),
        ],
        compiler_params=pltpu.CompilerParams(
            collective_id=0, has_side_effects=True, vmem_limit_bytes=16 << 20
        ),
        name="gram",
    )(snapshots, start.T)
    modes, operator, coefficients = pl.pallas_call(
        functools.partial(chain_kernel, cells * sizes[0] * sizes[1]),
        out_shape=(
            jax.ShapeDtypeStruct((order, cells), jnp.float32),
            jax.ShapeDtypeStruct((order, order), jnp.float32),
            jax.ShapeDtypeStruct((count, order), jnp.float32),
        ),
        in_specs=[vmem] * 3,
        out_specs=(vmem,) * 3,
        scratch_shapes=[pltpu.VMEM((padded, order), jnp.float32), pltpu.VMEM((padded, padded), jnp.float32)],
        compiler_params=pltpu.CompilerParams(vmem_limit_bytes=20 << 20),
        name="chain",
    )(snapshots, packed, right)
    return modes, operator, coefficients.T


def solution(mesh):
    def body(snapshots, start):
        return shards((mesh.shape["rows"], mesh.shape["sub"]), snapshots, start)

    return jax.shard_map(
        body,
        mesh=mesh,
        in_specs=(P(None, ("rows", "sub")), P()),
        out_specs=(P(None, ("rows", "sub")), P(), P()),
        check_vma=False,
    )
```
